16 devices in a mesh: dp: 2 (over y, z), tp: 8 (over x, core).
Axes of the slice: x: 4, y: 2, z: 1, core: 2. Of those that a mesh axis runs over, the one named last changes fastest.
The devices are a block of a 4x4x8 slice.
Arguments:
- x: bfloat16 [4096, 5120], P('dp'), parts along dimension 0
- gain: bfloat16 [5120], replicated
- wq: bfloat16 [5120, 8192], P(None, 'tp')
- wk: bfloat16 [5120, 1024], P(None, 'tp')
- wv: bfloat16 [5120, 1024], P(None, 'tp')
- wo: bfloat16 [8192, 5120], P('tp')
Outputs:
- output: bfloat16 [4096, 5120], P('dp'), parts along dimension 0
There are 2 independent parts. The reference program is written for one: setup_inputs(seed, part) draws one part's arguments, and reference() takes and returns one part's arrays. A program takes and returns all parts, laid end to end along the dimension named above; an argument that names none is the same for every part.
All inputs are finite; a program needn't handle non-finite values.
Results may differ from the reference program's by a relative error of at most 0.012.
Values are sent between devices in bfloat16 or wider.
A program may use at most 768 MiB of HBM per device.

```python
import jax
import jax.numpy as jnp
from jax import lax

ROWS = 2048
D = 5120
HEADS = 64
KV_HEADS = 8
HEAD = 128
THETA = 10000


def setup_inputs(seed: int = 0, part: int = 0) -> dict:
    kx, kn, kq, kk, kv, ko = jax.random.split(jax.random.key(seed), 6)

    def weights(key, rows, columns):
        return jax.random.normal(key, (rows, columns), jnp.float32) * rows**-0.5

    drawn = {
        "x": jax.random.normal(jax.random.fold_in(kx, part), (ROWS, D), jnp.float32),
        "gain": 1 + 0.1 * jax.random.normal(kn, (D,), jnp.float32),
        "wq": 2 * weights(kq, D, HEADS * HEAD),
        "wk": 2 * weights(kk, D, KV_HEADS * HEAD),
        "wv": 4 * weights(kv, D, KV_HEADS * HEAD),
        "wo": weights(ko, HEADS * HEAD, D),
    }
    return {k: v.astype(jnp.bfloat16) for k, v in drawn.items()}


def normed(x, gain):
    wide = x.astype(jnp.float32)
    scale = lax.rsqrt(jnp.mean(wide * wide, -1, keepdims=True) + 1e-6)
    return (wide * scale * gain.astype(jnp.float32)).astype(jnp.bfloat16)


def turned(t, place, theta):
    half = t.shape[-1] // 2
    angle = place.astype(jnp.float32)[:, None] * theta ** (-jnp.arange(half, dtype=jnp.float32) / half)
    cos, sin = jnp.cos(angle)[:, None], jnp.sin(angle)[:, None]
    a, b = t[..., :half].astype(jnp.float32), t[..., half:].astype(jnp.float32)
    return jnp.concatenate([a * cos - b * sin, b * cos + a * sin], -1).astype(jnp.bfloat16)


def matmul(a, w):
    return jnp.dot(a, w, preferred_element_type=jnp.float32).astype(jnp.bfloat16)


def einsum(form, a, b):
    return jnp.einsum(form, a.astype(jnp.float32), b.astype(jnp.float32))


def attention(q, k, v):
    scores = einsum("tgsd,ugd->gstu", q, k) * q.shape[-1] ** -0.5
    token = jnp.arange(q.shape[0])
    scores = jnp.where(token[:, None] >= token, scores, -jnp.inf)
    weights = jax.nn.softmax(scores, -1).astype(jnp.bfloat16)
    return einsum("gstu,ugd->tgsd", weights, v).astype(jnp.bfloat16)


def reference(x, gain, wq, wk, wv, wo):
    a, place = normed(x, gain), jnp.arange(ROWS)
    q = turned(matmul(a, wq).reshape(ROWS, HEADS, HEAD), place, THETA).reshape(ROWS, KV_HEADS, -1, HEAD)
    k = turned(matmul(a, wk).reshape(ROWS, KV_HEADS, HEAD), place, THETA)
    v = matmul(a, wv).reshape(ROWS, KV_HEADS, HEAD)
    seen = attention(q, k, v).reshape(ROWS, HEADS * HEAD)
    return (x.astype(jnp.float32) + jnp.dot(seen, wo, preferred_element_type=jnp.float32)).astype(jnp.bfloat16)
```

```python
import functools

import jax
import jax.numpy as jnp
import numpy as np
from jax import lax
from jax.experimental import pallas as pl
from jax.experimental.pallas import tpu as pltpu
from jax.sharding import PartitionSpec as P

HEAD = 128
THETA = 10000
HIDDEN = -2e30
LOG2E = 1.4426950408889634
VMEM = 64 * 2**20 - 2**16
BF16, F32 = jnp.bfloat16, jnp.float32
MESH = pl.DeviceIdType.MESH

CHUNK = 256
STRIP = 512
SLOTS = 4
PARTS = 4
NORM = 32


def _dot(a, b, ca, cb):
    return lax.dot_general(a, b, (((ca,), (cb,)), ((), ())), preferred_element_type=F32)


def _kernel(x_hbm, gain_ref, wq_hbm, wk_hbm, wv_hbm, wo_hbm, turn_hbm, out_hbm,
            wqkv, wo, xs, ks, vts, qs, top, mix, os, acc, pair_out, pair_in, a_out, a_in, b_out, b_in, keep, ys, xres, turn,
            w_sem, x_sem, t_sem, r_sem, po_sem, pi_sem, ao_sem, ai_sem, bo_sem, bi_sem,
            g_sem, gi_sem, f_sem, fi_sem, s_sem, si_sem, *, chips):
    rows, d = x_hbm.shape
    n = rows // CHUNK
    heads = wq_hbm.shape[1] // HEAD
    half, seg, piece = CHUNK // 2, CHUNK // 2 // chips, CHUNK // 4 // chips
    me = lax.axis_index("tp")
    chip, core = lax.div(me, 2), lax.rem(me, 2)
    at = lambda step: lax.rem(chip + step, chips)
    right = {"tp": at(1) * 2 + core}
    left = {"tp": at(chips - 1) * 2 + core}
    twin = {"tp": chip * 2 + 1 - core}

    barrier = pltpu.get_barrier_semaphore()
    for device in (right, left, twin):
        pl.semaphore_signal(barrier, inc=1, device_id=device, device_id_type=MESH)

    def send(src, dst, out_sem, in_sem, device):
        return pltpu.make_async_remote_copy(src_ref=src, dst_ref=dst, send_sem=out_sem, recv_sem=in_sem, device_id=device,
                                            device_id_type=MESH)

    def x_load(k):
        return pltpu.make_async_copy(x_hbm.at[pl.ds(pl.multiple_of(k * CHUNK, CHUNK), CHUNK)], xs.at[lax.rem(k, 2)], x_sem.at[lax.rem(k, 2)])

    def turn_load(k):
        return pltpu.make_async_copy(turn_hbm.at[pl.ds(pl.multiple_of(k * CHUNK, CHUNK), CHUNK)], turn.at[lax.rem(k, 2)], t_sem.at[lax.rem(k, 2)])

    hd = heads * HEAD
    w_loads = [pltpu.make_async_copy(wq_hbm, wqkv.at[:, :hd], w_sem.at[0]),
               pltpu.make_async_copy(wk_hbm, wqkv.at[:, hd : hd + HEAD], w_sem.at[1]),
               pltpu.make_async_copy(wv_hbm, wqkv.at[:, hd + HEAD :], w_sem.at[2])]
    wo_load = pltpu.make_async_copy(wo_hbm, wo, w_sem.at[3])
    x_load(0).start()
    turn_load(0).start()
    for load in w_loads:
        load.start()
    wo_load.start()
    pl.semaphore_wait(barrier, 3)

    blocks = [(c, min(1024, d - c)) for c in range(0, d, 1024)]


    def norm(k):
        s = lax.rem(k, 2)

        def some(r, _):
            here = pl.ds(pl.multiple_of(r * NORM, NORM), NORM)
            total = None
            for c, w in blocks:
                wide = xs[s, here, c : c + w].astype(F32)
                square = wide * wide
                for i in range(0, w, HEAD):
                    part = square[:, i : i + HEAD]
                    total = part if total is None else total + part
            scale = lax.rsqrt(jnp.sum(total, -1, keepdims=True) * (1 / d) + 1e-6)
            for c, w in blocks:
                wide = xs[s, here, c : c + w].astype(F32)
                xs[s, here, c : c + w] = (wide * scale * gain_ref[:, c : c + w].astype(F32)).astype(BF16)

        lax.fori_loop(0, CHUNK // NORM, some, None)

    def project(k):
        s = lax.rem(k, 2)
        both = turn[s]
        other = pltpu.roll(both, HEAD // 2, 1)
        low = lax.broadcasted_iota(jnp.int32, (CHUNK, HEAD), 1) < HEAD // 2
        cos = jnp.where(low, both, other)
        sin = jnp.where(low, -other, both)

        def turned(t):
            t = t.astype(BF16).astype(F32)
            return (t * cos + pltpu.roll(t, HEAD // 2, 1) * sin).astype(BF16)

        step = 2 * HEAD
        got = jnp.dot(xs[s], wqkv[:, hd : hd + step], preferred_element_type=F32)
        ks[pl.ds(pl.multiple_of(k * CHUNK, CHUNK), CHUNK), :] = turned(got[:, :HEAD])
        vts[k, :HEAD, :] = got[:, HEAD:].T.astype(BF16)
        vts[k, HEAD:, :] = jnp.ones((8, CHUNK), BF16)
        for h in range(0, heads, 2):
            got = jnp.dot(xs[s], wqkv[:, h * HEAD : h * HEAD + step], preferred_element_type=F32)
            for g in range(2):
                qs[(h + g) * CHUNK : (h + g + 1) * CHUNK, :] = turned(got[:, g * HEAD : (g + 1) * HEAD])

    cols = heads * CHUNK
    strips = list(range(0, cols, STRIP))
    e = HEAD**-0.5 * LOG2E

    def scored(j):
        key = ks[pl.ds(pl.multiple_of(j * CHUNK, CHUNK), CHUNK), :]
        return [_dot(key, qs[a : a + STRIP, :], 1, 1) for a in strips]

    def attend(k):
        value = vts[k]
        ok = (lax.broadcasted_iota(jnp.int32, (CHUNK, STRIP), 1) & (CHUNK - 1)) >= lax.broadcasted_iota(jnp.int32, (CHUNK, STRIP), 0)
        weights = []
        for a, sc in zip(strips, scored(k)):
            sc = jnp.where(ok, sc, HIDDEN)
            most = sc.max(axis=0, keepdims=True)
            top[:, a : a + STRIP] = most
            weights.append(jnp.exp2((sc - most) * e).astype(BF16))
        for a, p in zip(strips, weights):
            mix[:, a : a + STRIP] = _dot(value, p, 1, 0)

        def earlier(j, _):
            value = vts[j]
            weights, keeps = [], []
            for a, sc in zip(strips, scored(j)):
                old = top[:, a : a + STRIP]
                most = jnp.maximum(old, sc.max(axis=0, keepdims=True))
                top[:, a : a + STRIP] = most
                weights.append(jnp.exp2((sc - most) * e).astype(BF16))
                keeps.append(jnp.exp2((old - most) * e))
            for a, p, held in zip(strips, weights, keeps):
                mix[:, a : a + STRIP] = mix[:, a : a + STRIP] * held + _dot(value, p, 1, 0)

        lax.fori_loop(0, k, earlier, None)
        for h in range(heads):
            got = mix[:HEAD, h * CHUNK : (h + 1) * CHUNK] * (1 / mix[HEAD : HEAD + 1, h * CHUNK : (h + 1) * CHUNK])
            got = got.T.astype(BF16)
            for part in range(2):
                to = pl.ds(pl.multiple_of((core if part == 0 else 1 - core) * half, half), half)
                os[to, h * HEAD : (h + 1) * HEAD] = got[part * half : (part + 1) * half]

    width = d // PARTS

    def pair(k, g):
        there = pair_in.at[lax.rem(k, 2), :, g * width : (g + 1) * width]
        return send(pair_out.at[:, g * width : (g + 1) * width], there, po_sem.at[g], pi_sem.at[lax.rem(k, 2), g], twin)

    def project_out(k):
        step = 256
        for g in range(PARTS):
            for c in range(g * width, (g + 1) * width, step):
                got = jnp.dot(os[...], wo[:, c : c + step], preferred_element_type=F32)
                acc[:, c : c + step] = got[:half]
                pair_out[:, c : c + step] = got[half:].astype(BF16)
            pair(k, g).start()


    def stage_a(k, i):
        s, s2 = lax.rem(k, SLOTS), lax.rem(k, 2)
        return send(a_out.at[s2, i], a_in.at[s, i], ao_sem.at[s2, i], ai_sem.at[s, i], (right, left)[i % 2])

    def stage_b(k, i):
        s, s2 = lax.rem(k, SLOTS), lax.rem(k, 2)
        return send(b_out.at[s2, i], b_in.at[s, i], bo_sem.at[s2, i], bi_sem.at[s, i], (right, left)[i])

    def rows_of(k, which, step, size, off=0):
        return pl.ds(pl.multiple_of(k * CHUNK + which * half + at(step) * seg + off, piece), size)

    def residual(k):
        return pltpu.make_async_copy(x_hbm.at[rows_of(k, core, 0, seg)], xres.at[lax.rem(k, 2)], r_sem.at[lax.rem(k, 2)])

    def start_sum(k):
        s, s2 = lax.rem(k, SLOTS), lax.rem(k, 2)
        for g in range(PARTS):
            pair(k, g).wait_recv()
            c = slice(g * width, (g + 1) * width)

            def chip_sum(step, second):
                here = pl.ds(pl.multiple_of(at(step) * seg + second * piece, piece), piece)
                return acc[here, c] + pair_in[s2, here, c].astype(F32)

            a_out[s2, 0, :, c] = chip_sum(2, 0).astype(BF16)
            a_out[s2, 1, :, c] = chip_sum(2, 1).astype(BF16)
            a_out[s2, 2, :, c] = chip_sum(1, 1).astype(BF16)
            a_out[s2, 3, :, c] = chip_sum(chips - 1, 0).astype(BF16)
            keep[s, 0, :, c] = chip_sum(1, 0)
            keep[s, 1, :, c] = chip_sum(chips - 1, 1)
            keep[s, 2, :, c] = chip_sum(0, 0)
            keep[s, 3, :, c] = chip_sum(0, 1)
        for i in range(4):
            stage_a(k, i).start()
        for g in range(PARTS):
            pair(k, g).wait_send()

    def hand_on(k):
        s, s2 = lax.rem(k, SLOTS), lax.rem(k, 2)
        residual(k).start()
        for i in range(2):
            stage_a(k, i).wait_recv()
            for c, w in blocks:
                b_out[s2, i, :, c : c + w] = (keep[s, i, :, c : c + w] + a_in[s, i, :, c : c + w].astype(F32)).astype(BF16)
            stage_b(k, i).start()
        for i in range(4):
            stage_a(k, i).wait_send()

    def gather(k, i):
        s = lax.rem(k, SLOTS)
        there = out_hbm.at[rows_of(k, core, 0, seg)]
        if i == 2:
            return send(ys.at[s], there, g_sem.at[s, i], si_sem.at[k, 0], twin)
        return send(ys.at[s], there, g_sem.at[s, i], gi_sem.at[k, i], (right, left)[i])

    def own(k):
        s = lax.rem(k, SLOTS)
        return pltpu.make_async_copy(ys.at[s], out_hbm.at[rows_of(k, core, 0, seg)], g_sem.at[s, 3])

    def finish(k):
        s, s2 = lax.rem(k, SLOTS), lax.rem(k, 2)
        residual(k).wait()
        stage_a(k, 2).wait_recv()
        stage_a(k, 3).wait_recv()
        for i in range(2):
            stage_b(k, i).wait_recv()
            for c, w in blocks:
                total = keep[s, 2 + i, :, c : c + w] + b_in[s, i, :, c : c + w].astype(F32) + a_in[s, 3 - i, :, c : c + w].astype(F32)
                mine = xres[s2, i * piece : (i + 1) * piece, c : c + w].astype(F32)
                ys[s, i * piece : (i + 1) * piece, c : c + w] = (mine + total).astype(BF16)
        for i in range(3):
            gather(k, i).start()
        own(k).start()
        for i in range(2):
            stage_b(k, i).wait_send()

    def landed(ref, sem):
        return send(ref, ref, sem, sem, twin)

    def onward(k, i):
        here = out_hbm.at[rows_of(k, core, chips - 1 if i == 0 else 1, piece, i * piece)]
        return send(here, here, f_sem.at[lax.rem(k, SLOTS), i], fi_sem.at[k, i], (right, left)[i])

    def share(k, i):
        here = out_hbm.at[rows_of(k, core, (chips - 1, 1, 2)[i], seg)]
        return send(here, here, s_sem.at[lax.rem(k, SLOTS), i], si_sem.at[k, 1 + i], twin)

    def pass_on(k):
        for i in range(2):
            landed(out_hbm.at[rows_of(k, core, chips - 1 if i == 0 else 1, seg)], gi_sem.at[k, i]).wait_recv()
            onward(k, i).start()
            share(k, i).start()
        for i in range(3):
            gather(k, i).wait_send()
        own(k).wait()

    def pass_last(k):
        for i in range(2):
            landed(out_hbm.at[rows_of(k, core, 2, piece, i * piece)], fi_sem.at[k, i]).wait_recv()
        share(k, 2).start()
        for i in range(2):
            onward(k, i).wait_send()

    def close(k):
        for i in range(3):
            share(k, i).wait_send()
        for i, step in enumerate((0, chips - 1, 1, 2)):
            landed(out_hbm.at[rows_of(k, 1 - core, step, seg)], si_sem.at[k, i]).wait_recv()

    def step(i, _):
        @pl.when(i < n)
        def _():
            @pl.when(i + 1 < n)
            def _():
                x_load(i + 1).start()
                turn_load(i + 1).start()

            x_load(i).wait()
            norm(i)
            turn_load(i).wait()

            @pl.when(i == 0)
            def _():
                for load in w_loads:
                    load.wait()

            project(i)
            attend(i)

            @pl.when(i == 0)
            def _():
                wo_load.wait()

            project_out(i)
            start_sum(i)

        for late, stage in enumerate((hand_on, finish, pass_on, pass_last, close), 1):

            @pl.when((i >= late) & (i < n + late))
            def _(stage=stage, late=late):
                stage(i - late)

    lax.fori_loop(0, n + 5, step, None)


def solution(mesh):
    chips = mesh.shape["tp"] // 2

    def step(x, gain, wq, wk, wv, wo):
        rows, d = x.shape
        hd = wq.shape[1]
        n, heads = rows // CHUNK, hd // HEAD
        piece, seg, half = CHUNK // 4 // chips, CHUNK // 2 // chips, CHUNK // 2
        angle = np.arange(rows, dtype=np.float32)[:, None] * np.float32(THETA) ** (-np.arange(HEAD // 2, dtype=np.float32) / (HEAD // 2))
        turn = jnp.asarray(np.concatenate([np.cos(angle), np.sin(angle)], 1), F32)
        dma = lambda *shape: pltpu.SemaphoreType.DMA(shape)
        flops = 2 * rows * d * (hd + 2 * HEAD) + 2 * rows * hd * d + 2 * rows * rows * hd
        hbm = pl.BlockSpec(memory_space=pl.ANY)
        return pl.pallas_call(
            functools.partial(_kernel, chips=chips),
            out_shape=jax.ShapeDtypeStruct((rows, d), BF16),
            in_specs=[hbm, pl.BlockSpec(memory_space=pltpu.VMEM)] + [hbm] * 5,
            out_specs=hbm,
            scratch_shapes=[
                pltpu.VMEM((d, hd + 2 * HEAD), BF16),
                pltpu.VMEM((hd, d), BF16),
                pltpu.VMEM((2, CHUNK, d), BF16),
                pltpu.VMEM((rows, HEAD), BF16),
                pltpu.VMEM((n, HEAD + 8, CHUNK), BF16),
                pltpu.VMEM((heads * CHUNK, HEAD), BF16),
                pltpu.VMEM((1, heads * CHUNK), F32),
                pltpu.VMEM((HEAD + 8, heads * CHUNK), F32),
                pltpu.VMEM((CHUNK, hd), BF16),
                pltpu.VMEM((half, d), F32),
                pltpu.VMEM((half, d), BF16),
                pltpu.VMEM((2, half, d), BF16),
                pltpu.VMEM((2, 4, piece, d), BF16),
                pltpu.VMEM((SLOTS, 4, piece, d), BF16),
                pltpu.VMEM((2, 2, piece, d), BF16),
                pltpu.VMEM((SLOTS, 2, piece, d), BF16),
                pltpu.VMEM((SLOTS, 4, piece, d), F32),
                pltpu.VMEM((SLOTS, seg, d), BF16),
                pltpu.VMEM((2, seg, d), BF16),
                pltpu.VMEM((2, CHUNK, HEAD), F32),
                dma(4), dma(2), dma(2), dma(2),
                dma(PARTS), dma(2, PARTS),
                dma(2, 4), dma(SLOTS, 4), dma(2, 2), dma(SLOTS, 2),
                dma(SLOTS, 4), dma(n, 2), dma(SLOTS, 2), dma(n, 2), dma(SLOTS, 3), dma(n, 4),
            ],
            compiler_params=pltpu.CompilerParams(collective_id=0, has_side_effects=True, vmem_limit_bytes=VMEM),
            cost_estimate=pl.CostEstimate(flops=flops, transcendentals=rows * rows * heads // 2,
                                          bytes_accessed=2 * (2 * rows * d + d * (2 * hd + 2 * HEAD))),
        )(x, gain.reshape(1, d), wq, wk, wv, wo, turn)

    tokens, columns = P("dp", None), P(None, "tp")
    return jax.shard_map(
        step,
        mesh=mesh,
        in_specs=(tokens, P(None), columns, columns, columns, P("tp", None)),
        out_specs=tokens,
        check_vma=False,
    )
```
